64 devices in a mesh: dp: 4 (over x, y), sp: 16 (over z, core).
Axes of the slice: x: 2, y: 2, z: 8, core: 2. Of those that a mesh axis runs over, the one named last changes fastest.
The devices are a block of a 4x4x8 slice.
Arguments:
- hidden: bfloat16 [128, 512, 2048], P('dp', 'sp'), parts along dimension 0
- seq_lens: int32 [128], P('dp'), parts along dimension 0
- ln1_gain: float32 [2048], replicated
- ln1_bias: float32 [2048], replicated
- ln2_gain: float32 [2048], replicated
- ln2_bias: float32 [2048], replicated
- w_qkv: bfloat16 [2048, 6144], replicated
- b_qkv: float32 [16, 3, 128], replicated
- w_out: bfloat16 [2048, 2048], replicated
- b_out: float32 [2048], replicated
- w_up: bfloat16 [2048, 8192], replicated
- b_up: float32 [8192], replicated
- w_down: bfloat16 [8192, 2048], replicated
- b_down: float32 [2048], replicated
Outputs:
- output 1: bfloat16 [128, 512, 2048], P('dp', 'sp'), parts along dimension 0
- output 2: bfloat16 [128, 16, 512, 128], P('dp', 'sp'), parts along dimension 0
- output 3: bfloat16 [128, 16, 512, 128], P('dp', 'sp'), parts along dimension 0
There are 4 independent parts. The reference program is written for one: setup_inputs(seed, part) draws one part's arguments, and reference() takes and returns one part's arrays. A program takes and returns all parts, laid end to end along the dimension named above; an argument that names none is the same for every part.
All inputs are finite; a program needn't handle non-finite values.
Results may differ from the reference program's by a relative error of at most 0.00254755.
Values are sent between devices in bfloat16 or wider.
A program may use at most 768 MiB of HBM per device.

```python
import jax
import jax.numpy as jnp
from jax import lax

BATCH_SEQS = 32
SEQ_SHARDS = 16
ROWS_DEV = 32
D_MODEL = 2048
N_HEADS = 16
HEAD_DIM = 128
D_FF = 8192

SEQ_LEN = ROWS_DEV * SEQ_SHARDS
ROT_DIM = HEAD_DIM // 4
LN_EPS = 1e-5
ROT_BASE = 10000.0


def setup_inputs(seed: int = 0, part: int = 0) -> dict:
    part_key = jax.random.fold_in(jax.random.key(seed), part)
    shared = jax.random.split(jax.random.key(seed + 7919), 12)
    key_x, key_len, key_full = jax.random.split(part_key, 3)
    hidden = jax.random.normal(key_x, (BATCH_SEQS, SEQ_LEN, D_MODEL), jnp.float32).astype(jnp.bfloat16)
    drawn = jax.random.randint(key_len, (BATCH_SEQS,), SEQ_LEN // 2 + 1, SEQ_LEN + 1, jnp.int32)
    full_row = jax.random.randint(key_full, (), 0, BATCH_SEQS, jnp.int32)
    seq_lens = jnp.where(jnp.arange(BATCH_SEQS) == full_row, SEQ_LEN, drawn).astype(jnp.int32)

    def gauss(key, shape, scale):
        return jax.random.normal(key, shape, jnp.float32) * scale

    return {
        'hidden': hidden,
        'seq_lens': seq_lens,
        'ln1_gain': 1.0 + gauss(shared[0], (D_MODEL,), 0.2),
        'ln1_bias': gauss(shared[1], (D_MODEL,), 0.2),
        'ln2_gain': 1.0 + gauss(shared[2], (D_MODEL,), 0.2),
        'ln2_bias': gauss(shared[3], (D_MODEL,), 0.2),
        'w_qkv': gauss(shared[4], (D_MODEL, 3 * D_MODEL), 1.5 * D_MODEL ** -0.5).astype(jnp.bfloat16),
        'b_qkv': gauss(shared[5], (N_HEADS, 3, HEAD_DIM), 0.3),
        'w_out': gauss(shared[6], (D_MODEL, D_MODEL), D_MODEL ** -0.5).astype(jnp.bfloat16),
        'b_out': gauss(shared[7], (D_MODEL,), 0.3),
        'w_up': gauss(shared[8], (D_MODEL, D_FF), D_MODEL ** -0.5).astype(jnp.bfloat16),
        'b_up': gauss(shared[9], (D_FF,), 0.3),
        'w_down': gauss(shared[10], (D_FF, D_MODEL), 1.5 * D_FF ** -0.5).astype(jnp.bfloat16),
        'b_down': gauss(shared[11], (D_MODEL,), 0.3),
    }


def layer_norm(rows, gain, shift):
    rows32 = rows.astype(jnp.float32)
    centered = rows32 - jnp.mean(rows32, axis=-1, keepdims=True)
    variance = jnp.mean(centered * centered, axis=-1, keepdims=True)
    return (centered * lax.rsqrt(variance + LN_EPS) * gain + shift).astype(jnp.bfloat16)


def rotary(vecs, positions):
    half_rot = ROT_DIM // 2
    inv_freq = ROT_BASE ** (-2.0 * jnp.arange(half_rot, dtype=jnp.float32) / ROT_DIM)
    angles = positions.astype(jnp.float32)[:, None] * inv_freq[None, :]
    cosines = jnp.cos(angles)[:, None, :]
    sines = jnp.sin(angles)[:, None, :]
    first = vecs[..., :half_rot]
    second = vecs[..., half_rot:ROT_DIM]
    return jnp.concatenate([first * cosines - second * sines, second * cosines + first * sines, vecs[..., ROT_DIM:]], axis=-1)


def reference(hidden, seq_lens, ln1_gain, ln1_bias, ln2_gain, ln2_bias, w_qkv, b_qkv, w_out, b_out, w_up, b_up, w_down, b_down):
    n_blocks = BATCH_SEQS * SEQ_SHARDS
    row_blocks = hidden.reshape(n_blocks, ROWS_DEV, D_MODEL)
    block_start = (jnp.arange(n_blocks) % SEQ_SHARDS) * ROWS_DEV

    def project(operands):
        rows, start = operands
        normed = layer_norm(rows, ln1_gain, ln1_bias)
        proj_qkv = jnp.dot(normed, w_qkv, preferred_element_type=jnp.float32)
        proj_qkv = proj_qkv.reshape(ROWS_DEV, N_HEADS, 3, HEAD_DIM) + b_qkv
        positions = start + jnp.arange(ROWS_DEV)
        q_rows = rotary(proj_qkv[:, :, 0], positions).astype(jnp.bfloat16)
        k_rows = rotary(proj_qkv[:, :, 1], positions).astype(jnp.bfloat16)
        v_rows = proj_qkv[:, :, 2].astype(jnp.bfloat16)
        return q_rows, k_rows, v_rows

    q_all, k_all, v_all = lax.map(project, (row_blocks, block_start))
    q_heads = jnp.transpose(q_all.reshape(BATCH_SEQS, SEQ_LEN, N_HEADS, HEAD_DIM), (2, 0, 1, 3))
    k_cache = jnp.transpose(k_all.reshape(BATCH_SEQS, SEQ_LEN, N_HEADS, HEAD_DIM), (0, 2, 1, 3))
    v_cache = jnp.transpose(v_all.reshape(BATCH_SEQS, SEQ_LEN, N_HEADS, HEAD_DIM), (0, 2, 1, 3))
    key_pos = jnp.arange(SEQ_LEN)
    score_scale = HEAD_DIM ** -0.5

    def one_head(operands):
        q_one, k_one, v_one = operands
        k_wide = k_one.astype(jnp.float32)
        v_wide = v_one.astype(jnp.float32)

        def one_block(start):
            q_blk = lax.dynamic_slice_in_dim(q_one, start, ROWS_DEV, axis=1).astype(jnp.float32)
            scores = jnp.einsum('bqd,bkd->bqk', q_blk, k_wide) * score_scale
            q_pos = start + jnp.arange(ROWS_DEV)
            allowed = (key_pos[None, None, :] <= q_pos[None, :, None]) & (key_pos[None, None, :] < seq_lens[:, None, None])
            scores = jnp.where(allowed, scores, -jnp.inf)
            weights = jnp.exp(scores - jnp.max(scores, axis=-1, keepdims=True))
            total = jnp.sum(weights, axis=-1, keepdims=True)
            rounded = weights.astype(jnp.bfloat16).astype(jnp.float32)
            context = jnp.einsum('bqk,bkd->bqd', rounded, v_wide) / total
            return context.astype(jnp.bfloat16)

        blocks = lax.map(one_block, jnp.arange(SEQ_SHARDS) * ROWS_DEV)
        return jnp.transpose(blocks, (1, 0, 2, 3)).reshape(BATCH_SEQS, SEQ_LEN, HEAD_DIM)

    k_for_heads = jnp.transpose(k_cache, (1, 0, 2, 3))
    v_for_heads = jnp.transpose(v_cache, (1, 0, 2, 3))
    context = lax.map(one_head, (q_heads, k_for_heads, v_for_heads))
    ctx_blocks = jnp.transpose(context, (1, 2, 0, 3)).reshape(n_blocks, ROWS_DEV, D_MODEL)

    def finish(operands):
        rows, ctx_rows = operands
        attn_out = jnp.dot(ctx_rows, w_out, preferred_element_type=jnp.float32) + b_out
        normed = layer_norm(rows, ln2_gain, ln2_bias)
        pre_act = jnp.dot(normed, w_up, preferred_element_type=jnp.float32) + b_up
        hidden_act = jax.nn.gelu(pre_act, approximate=False).astype(jnp.bfloat16)
        mlp_out = jnp.dot(hidden_act, w_down, preferred_element_type=jnp.float32) + b_down
        return (rows.astype(jnp.float32) + attn_out + mlp_out).astype(jnp.bfloat16)

    out_blocks = lax.map(finish, (row_blocks, ctx_blocks))
    return out_blocks.reshape(BATCH_SEQS, SEQ_LEN, D_MODEL), k_cache, v_cache
```

```python
import functools

import jax
import jax.numpy as jnp
import numpy as np
from jax import lax
from jax.experimental import pallas as pl
from jax.experimental.pallas import tpu as pltpu
from jax.sharding import PartitionSpec as P

LN_EPS = 1e-5
ROT_BASE = 10000.0
PC = 4
AHEAD = 3
FB = 512
MESH = pl.DeviceIdType.MESH
VMEM_LIMIT = 66_900_000
ANY = pl.BlockSpec(memory_space=pl.ANY)
VM = pl.BlockSpec(memory_space=pltpu.VMEM)
SM = pl.BlockSpec(memory_space=pltpu.SMEM)


def rotary_tables(seq_len, head_dim):
    rot = head_dim // 4
    half = rot // 2
    inv = np.float32(ROT_BASE) ** (np.float32(-2.0) * np.arange(half, dtype=np.float32) / np.float32(rot))
    ang = np.arange(seq_len, dtype=np.float32)[:, None] * inv[None, :].astype(np.float32)
    cos, sin = np.cos(ang), np.sin(ang)
    c = np.ones((seq_len, head_dim), np.float32)
    s = np.zeros((2, seq_len, head_dim), np.float32)
    c[:, :half] = cos
    c[:, half:rot] = cos
    s[0, :, :half] = -sin
    s[1, :, half:rot] = sin
    return c, s[0], s[1]


def entry_barrier(n, me):
    sem = pltpu.get_barrier_semaphore()
    for d in range(1, n):
        pl.semaphore_signal(sem, inc=1, device_id={'sp': lax.rem(me + d, n)}, device_id_type=MESH)
    return lambda: pl.semaphore_wait(sem, n - 1)


def project_kernel(n, hid, g1, s1, g2, s2, wqkv, bqkv, tab_c, tab_l, tab_r, wup, bup, wdn, bsum,
                   q_out, k_out, v_out, acc_out,
                   a_own, a_nb, m_buf, acc, w_sc, wup_b, wdn_b, st,
                   x_sem, w_sem, up_sem, dn_sem, a_send, a_recv, st_sem, self_sem, r_sem, o_sem):
    me = lax.axis_index('sp')
    chip = lax.div(me, 2)
    n_prompts, tok, d_model = hid.shape
    hd = q_out.shape[3]
    wide = 3 * hd
    n_chunks = n_prompts // PC
    rows = PC * tok
    n_far = n // 2 - 3
    n_loc = n_far + 2
    n_w = 2 * n_far + 2
    n_fb = bup.shape[0]
    fb = bup.shape[2]
    outs = (q_out, k_out, v_out)

    await_barrier = entry_barrier(n, me)

    def x_copy(i):
        r = pl.multiple_of(i * rows, rows)
        return pltpu.make_async_copy(hid.at[pl.ds(i * PC, PC)], m_buf.at[pl.ds(i * PC, PC)], x_sem.at[i])

    def w_copy(j):
        head = lax.rem(2 * chip - n_far + j + n, n)
        return pltpu.make_async_copy(wqkv.at[:, pl.ds(pl.multiple_of(head * wide, 128), wide)], w_sc.at[j], w_sem.at[j])

    def up_copy(j, slot):
        return pltpu.make_async_copy(wup.at[:, pl.ds(pl.multiple_of(j * fb, 128), fb)], wup_b.at[slot], up_sem.at[slot])

    def dn_copy(j, slot):
        return pltpu.make_async_copy(wdn.at[pl.ds(pl.multiple_of(j * fb, 128), fb)], wdn_b.at[slot], dn_sem.at[slot])

    @pl.loop(0, n_chunks)
    def _(i):
        x_copy(i).start()

    @pl.loop(0, n_w)
    def _(j):
        w_copy(j).start()

    for j in range(2):
        up_copy(j, j).start()
        dn_copy(j, j).start()

    def a_copy(side, i):
        to = lax.rem(me + (2 if side == 0 else n - 2), n)
        r = pl.ds(pl.multiple_of(i * rows, rows), rows)
        return pltpu.make_async_remote_copy(
            src_ref=a_own.at[r], dst_ref=a_nb.at[side, r], send_sem=a_send.at[side, i], recv_sem=a_recv.at[side, i],
            device_id={'sp': to}, device_id_type=MESH)

    def norm_chunk(i):
        x_copy(i).wait()
        r = pl.ds(pl.multiple_of(i * rows, rows), rows)
        pr = pl.ds(i * PC, PC)
        x = m_buf[pr].reshape(rows, d_model).astype(jnp.float32)
        cen = x - jnp.mean(x, axis=-1, keepdims=True)
        var = jnp.mean(cen * cen, axis=-1, keepdims=True)
        nor = cen * lax.rsqrt(var + LN_EPS)
        a_own[r] = (nor * g1[...] + s1[...]).astype(jnp.bfloat16)
        m_buf[pr] = (nor * g2[...] + s2[...]).astype(jnp.bfloat16).reshape(PC, tok, d_model)
        acc[r] = x + bsum[...]

    norm_chunk(0)
    await_barrier()
    for side in range(2):
        a_copy(side, 0).start()

    @pl.loop(1, n_chunks)
    def _(i):
        norm_chunk(i)

        @pl.when(i < AHEAD)
        def _():
            for side in range(2):
                a_copy(side, i).start()

    @pl.loop(0, n_w)
    def _(j):
        w_copy(j).wait()

    def finish_block(y, head, src, slot, blk):
        y = y + bqkv[head]
        t = pl.ds(pl.multiple_of(src * tok, tok), tok)
        cc, cl, cr = tab_c[t][None], tab_l[t][None], tab_r[t][None]
        for m in range(3):
            u = y[:, m * hd:(m + 1) * hd]
            if m < 2:
                far = pltpu.roll(u, hd - hd // 8, 1).reshape(PC, tok, hd)
                near = pltpu.roll(u, hd // 8, 1).reshape(PC, tok, hd)
                u = u.reshape(PC, tok, hd) * cc + far * cl + near * cr
            else:
                u = u.reshape(PC, tok, hd)
            st[slot, blk, m] = u.astype(jnp.bfloat16)

    def place(m, i, src):
        return outs[m].at[pl.ds(i * PC, PC), 0, pl.ds(pl.multiple_of(src * tok, tok), tok)]

    def send_block(i, src, slot, blk, dest):
        for m in range(3):
            pltpu.make_async_remote_copy(
                src_ref=st.at[slot, blk, m], dst_ref=place(m, i, src), send_sem=st_sem.at[slot], recv_sem=r_sem.at[m, i],
                device_id={'sp': dest}, device_id_type=MESH).start()

    n_remote = 2 * n_far + 3

    def free_slot(slot):
        pltpu.make_async_copy(st.at[slot, pl.ds(0, n_remote)], st.at[slot, pl.ds(0, n_remote)], st_sem.at[slot]).wait()
        pltpu.make_async_copy(st.at[slot, pl.ds(0, 3)], st.at[slot, pl.ds(0, 3)], self_sem.at[slot]).wait()

    def mlp_block(j):
        slot = lax.rem(j, 2)
        up_copy(j, slot).wait()
        dn_copy(j, slot).wait()
        mp = 4 * PC

        @pl.loop(0, n_prompts // mp)
        def _(r):
            rr = pl.ds(pl.multiple_of(r * mp * tok, mp * tok), mp * tok)
            x = m_buf[pl.ds(r * mp, mp)].reshape(mp * tok, d_model)
            pre = jnp.dot(x, wup_b[slot], preferred_element_type=jnp.float32) + bup[j]
            act = (0.5 * pre * (1.0 + lax.erf(pre * np.float32(np.sqrt(0.5))))).astype(jnp.bfloat16)
            acc[rr] += jnp.dot(act, wdn_b[slot], preferred_element_type=jnp.float32)

        @pl.when(j + 2 < n_fb)
        def _():
            up_copy(j + 2, slot).start()
            dn_copy(j + 2, slot).start()

    below = lax.rem(me + n - 2, n)
    above = lax.rem(me + 2, n)
    per_tick = n_fb // n_chunks

    @pl.loop(0, n_chunks)
    def _(i):
        slot = lax.rem(i, 2)
        r = pl.ds(pl.multiple_of(i * rows, rows), rows)

        @pl.when(i + AHEAD < n_chunks)
        def _():
            for side in range(2):
                a_copy(side, i + AHEAD).start()

        for side in range(2):
            a_copy(side, i).wait_recv()

        @pl.when(i >= 2)
        def _():
            free_slot(slot)

        @pl.loop(0, n_far)
        def _(t):
            jl = n_w - 1 - t
            hl = lax.rem(2 * chip - n_far + jl + n, n)
            y = jnp.dot(a_nb[0, r], w_sc[jl], preferred_element_type=jnp.float32)
            finish_block(y, hl, below, slot, t)
            send_block(i, below, slot, t, hl)
            hr = lax.rem(2 * chip - n_far + t + n, n)
            y = jnp.dot(a_nb[1, r], w_sc[t], preferred_element_type=jnp.float32)
            finish_block(y, hr, above, slot, n_far + t)
            send_block(i, above, slot, n_far + t, hr)

        @pl.loop(0, 2)
        def _(q):
            dest = 2 * chip + jnp.where(q == 1, lax.rem(me, 2), 1 - lax.rem(me, 2))
            j = dest - 2 * chip + n_far
            for g, src in enumerate((below, me, above)):
                rows_in = a_own[r] if g == 1 else a_nb[g // 2, r]
                y = jnp.dot(rows_in, w_sc[j], preferred_element_type=jnp.float32)
                finish_block(y, dest, src, slot, 2 * n_far + 3 * q + g)

            @pl.when(q == 0)
            def _():
                for g, src in enumerate((below, me, above)):
                    send_block(i, src, slot, 2 * n_far + g, dest)

            @pl.when(q == 1)
            def _():
                for g, src in enumerate((below, me, above)):
                    for m in range(3):
                        pltpu.make_async_copy(st.at[slot, n_remote + g, m], place(m, i, src), self_sem.at[slot]).start()

        @pl.loop(0, per_tick)
        def _(j):
            mlp_block(i * per_tick + j)

    out_copy = pltpu.make_async_copy(acc, acc_out, o_sem)
    out_copy.start()

    for slot in range(2):
        free_slot(slot)

    @pl.loop(0, n_chunks)
    def _(i):
        for side in range(2):
            a_copy(side, i).wait_send()
        for m in range(3):
            got = outs[m].at[pl.ds(0, PC), 0, pl.ds(0, (n - 3) * tok)]
            pltpu.make_async_copy(got, got, r_sem.at[m, i]).wait()

    out_copy.wait()


def attend_kernel(n, lens, q_in, k_in, v_in, acc_in, wout, out,
                  qb, kb, vb, ctx_st, ctx_rv, w_b, acc, out_b,
                  in_sem, w_sem, acc_sem, send_sem, recv_sem, o_sem):
    me = lax.axis_index('sp')
    n_prompts, tok, d_model = out.shape
    seq, hd = q_in.shape[2], q_in.shape[3]
    n_chunks = n_prompts // PC
    rows = PC * tok
    scale = np.float32(hd ** -0.5)

    await_barrier = entry_barrier(n, me)

    def loads(i, slot):
        return [pltpu.make_async_copy(src.at[pl.ds(i * PC, PC), 0], dst.at[slot], in_sem.at[t, slot])
                for t, (src, dst) in enumerate(((q_in, qb), (k_in, kb), (v_in, vb)))]

    for i in range(2):
        for c in loads(i, i):
            c.start()
    w_copy = pltpu.make_async_copy(wout, w_b, w_sem)
    w_copy.start()
    acc_copy = pltpu.make_async_copy(acc_in, acc, acc_sem)
    acc_copy.start()
    await_barrier()

    blk = seq // 2

    @pl.loop(0, n_chunks)
    def _(i):
        slot = lax.rem(i, 2)
        for c in loads(i, slot):
            c.wait()

        @pl.loop(0, PC)
        def _(p):
            length = lens[i * PC + p]
            for b in range(2):
                keys = (b + 1) * blk
                q = qb[slot, p, b * blk:keys]
                k = kb[slot, p, :keys]
                v = vb[slot, p, :keys]
                s = lax.dot_general(q, k, (((1,), (1,)), ((), ())), preferred_element_type=jnp.float32) * scale
                key = lax.broadcasted_iota(jnp.int32, (blk, keys), 1)
                row = lax.broadcasted_iota(jnp.int32, (blk, keys), 0) + b * blk
                s = jnp.where((key <= row) & (key < length), s, -jnp.inf)
                w = jnp.exp(s - jnp.max(s, axis=-1, keepdims=True))
                z = jnp.sum(w, axis=-1, keepdims=True)
                c = jnp.dot(w.astype(jnp.bfloat16), v, preferred_element_type=jnp.float32) / z
                ctx_st[i * PC + p, b * blk:keys] = c.astype(jnp.bfloat16)

        @pl.when(i + 2 < n_chunks)
        def _():
            for c in loads(i + 2, slot):
                c.start()

        pr = pl.ds(i * PC, PC)
        for d in range(1, n):
            dest = lax.rem(me + d, n)
            pltpu.make_async_remote_copy(
                src_ref=ctx_st.at[pr, pl.ds(pl.multiple_of(dest * tok, tok), tok)], dst_ref=ctx_rv.at[me, pr],
                send_sem=send_sem, recv_sem=recv_sem.at[i], device_id={'sp': dest}, device_id_type=MESH).start()
        ctx_rv[me, pr] = ctx_st[pr, pl.ds(pl.multiple_of(me * tok, tok), tok)]

    w_copy.wait()
    acc_copy.wait()

    def store(i, slot):
        return pltpu.make_async_copy(out_b.at[slot], out.at[pl.ds(i * PC, PC)], o_sem.at[slot])

    @pl.loop(0, n_chunks)
    def _(i):
        slot = lax.rem(i, 2)
        pr = pl.ds(i * PC, PC)
        got = ctx_rv.at[pl.ds(0, n - 1), pl.ds(0, PC)]
        pltpu.make_async_copy(got, got, recv_sem.at[i]).wait()

        @pl.when(i >= 2)
        def _():
            store(i - 2, slot).wait()

        ctx = jnp.concatenate([ctx_rv[h, pr].reshape(rows, hd) for h in range(n)], axis=1)
        r = pl.ds(pl.multiple_of(i * rows, rows), rows)
        for t in range(4):
            cols = slice(t * (d_model // 4), (t + 1) * (d_model // 4))
            y = jnp.dot(ctx, w_b[:, cols], preferred_element_type=jnp.float32) + acc[r, cols]
            out_b[slot, :, :, cols] = y.astype(jnp.bfloat16).reshape(PC, tok, d_model // 4)
        store(i, slot).start()

    for i in range(2):
        store(n_chunks - 2 + i, (n_chunks + i) % 2).wait()
    sent = ctx_st.at[:, pl.ds(0, (n - 1) * tok)]
    pltpu.make_async_copy(sent, sent, send_sem).wait()


def solution(mesh):
    n = mesh.shape['sp']
    row_spec = P('dp', 'sp', None)
    cache_spec = P('dp', 'sp', None, None)
    vec_spec = P(None)
    mat_spec = P(None, None)

    def local_layer(hidden, seq_lens, ln1_gain, ln1_bias, ln2_gain, ln2_bias, w_qkv, b_qkv, w_out, b_out, w_up, b_up, w_down, b_down):
        n_prompts, tok, d_model = hidden.shape
        n_heads, _, hd = b_qkv.shape
        d_ff = w_up.shape[1]
        seq = tok * n
        n_rows = n_prompts * tok
        n_chunks = n_prompts // PC
        rows = PC * tok
        fb = min(FB, d_ff // n_chunks)
        n_far = n // 2 - 3
        bf, f32 = jnp.bfloat16, jnp.float32
        row = lambda v: v.reshape(1, d_model)
        tabs = [jnp.asarray(t) for t in rotary_tables(seq, hd)]
        cache = jax.ShapeDtypeStruct((n_prompts, 1, seq, hd), bf)
        dma = pltpu.SemaphoreType.DMA
        q, k, v, acc = pl.pallas_call(
            functools.partial(project_kernel, n),
            name='project',
            out_shape=(cache, cache, cache, jax.ShapeDtypeStruct((n_rows, d_model), f32)),
            in_specs=[ANY, VM, VM, VM, VM, ANY, VM, VM, VM, VM, ANY, VM, ANY, VM],
            out_specs=(ANY, ANY, ANY, ANY),
            scratch_shapes=[
                pltpu.VMEM((n_rows, d_model), bf),
                pltpu.VMEM((2, n_rows, d_model), bf),
                pltpu.VMEM((n_prompts, tok, d_model), bf),
                pltpu.VMEM((n_rows, d_model), f32),
                pltpu.VMEM((2 * n_far + 2, d_model, 3 * hd), bf),
                pltpu.VMEM((2, d_model, fb), bf),
                pltpu.VMEM((2, fb, d_model), bf),
                pltpu.VMEM((2, 2 * n_far + 6, 3, PC, tok, hd), bf),
                dma((n_chunks,)), dma((2 * n_far + 2,)), dma((2,)), dma((2,)), dma((2, n_chunks)), dma((2, n_chunks)),
                dma((2,)), dma((2,)), dma((3, n_chunks)), dma(()),
            ],
            compiler_params=pltpu.CompilerParams(collective_id=0, has_side_effects=True, vmem_limit_bytes=VMEM_LIMIT),
            cost_estimate=pl.CostEstimate(flops=2 * n_rows * d_model * (3 * d_model + 2 * d_ff), bytes_accessed=200_000_000, transcendentals=0),
        )(hidden, row(ln1_gain), row(ln1_bias), row(ln2_gain), row(ln2_bias), w_qkv, b_qkv.reshape(n_heads, 1, 3 * hd), *tabs,
          w_up, b_up.reshape(d_ff // fb, 1, fb), w_down, row(b_out + b_down))
        out = pl.pallas_call(
            functools.partial(attend_kernel, n),
            name='attend',
            out_shape=jax.ShapeDtypeStruct((n_prompts, tok, d_model), bf),
            in_specs=[SM, ANY, ANY, ANY, ANY, ANY],
            out_specs=ANY,
            scratch_shapes=[
                pltpu.VMEM((2, PC, seq, hd), bf), pltpu.VMEM((2, PC, seq, hd), bf), pltpu.VMEM((2, PC, seq, hd), bf),
                pltpu.VMEM((n_prompts, seq, hd), bf),
                pltpu.VMEM((n, n_prompts, tok, hd), bf),
                pltpu.VMEM((d_model, d_model), bf),
                pltpu.VMEM((n_rows, d_model), f32),
                pltpu.VMEM((2, PC, tok, d_model), bf),
                dma((3, 2)), dma(()), dma(()), dma(()), dma((n_chunks,)), dma((2,)),
            ],
            compiler_params=pltpu.CompilerParams(collective_id=1, has_side_effects=True, vmem_limit_bytes=VMEM_LIMIT),
            cost_estimate=pl.CostEstimate(flops=2 * n_rows * d_model * d_model, bytes_accessed=50_000_000, transcendentals=0),
        )(seq_lens, q, k, v, acc, w_out)
        return out, k, v

    return jax.shard_map(local_layer, mesh=mesh,
                         in_specs=(row_spec, P('dp'), vec_spec, vec_spec, vec_spec, vec_spec, mat_spec, P(None, None, None), mat_spec, vec_spec, mat_spec, vec_spec, mat_spec, vec_spec),
                         out_specs=(row_spec, cache_spec, cache_spec), check_vma=False)
```

```python
import functools

import jax
import jax.numpy as jnp
import numpy as np
from jax import lax
from jax.experimental import pallas as pl
from jax.experimental.pallas import tpu as pltpu
from jax.sharding import PartitionSpec as P

LN_EPS = 1e-5
ROT_BASE = 10000.0
PC = 4
AHEAD = 3
FB = 256
MESH = pl.DeviceIdType.MESH
VMEM_LIMIT = 66_900_000
ANY = pl.BlockSpec(memory_space=pl.ANY)
VM = pl.BlockSpec(memory_space=pltpu.VMEM)
SM = pl.BlockSpec(memory_space=pltpu.SMEM)


def rotary_tables(seq_len, head_dim):
    rot = head_dim // 4
    half = rot // 2
    inv = np.float32(ROT_BASE) ** (np.float32(-2.0) * np.arange(half, dtype=np.float32) / np.float32(rot))
    ang = np.arange(seq_len, dtype=np.float32)[:, None] * inv[None, :].astype(np.float32)
    cos, sin = np.cos(ang), np.sin(ang)
    c = np.ones((seq_len, head_dim), np.float32)
    s = np.zeros((2, seq_len, head_dim), np.float32)
    c[:, :half] = cos
    c[:, half:rot] = cos
    s[0, :, :half] = -sin
    s[1, :, half:rot] = sin
    return c, s[0], s[1]


def entry_barrier(n, me):
    sem = pltpu.get_barrier_semaphore()
    for d in range(1, n):
        pl.semaphore_signal(sem, inc=1, device_id={'sp': lax.rem(me + d, n)}, device_id_type=MESH)
    return lambda: pl.semaphore_wait(sem, n - 1)


def layer_kernel(n, lens, hid, g1, s1, g2, s2, wqkv, bqkv, tab_c, tab_l, tab_r, wup, bup, wdn, bdn, wout, bout,
                 q_out, k_out, v_out, out,
                 a_own, a_nb, m_buf, acc, w_sc, wup_b, wdn_b, st, qb, kb, vb, ctx_st, ctx_rv, out_b,
                 x_sem, w_sem, up_sem, dn_sem, a_send, a_recv, st_sem, self_sem, r_sem, in_sem, c_send, c_recv, wo_sem, o_sem):
    me = lax.axis_index('sp')
    chip = lax.div(me, 2)
    n_prompts, tok, d_model = hid.shape
    seq, hd = q_out.shape[2], q_out.shape[3]
    wide = 3 * hd
    n_chunks = n_prompts // PC
    rows = PC * tok
    n_far = n // 2 - 3
    n_w = 2 * n_far + 2
    n_remote = 2 * n_far + 3
    n_fb, fb = bup.shape[0], bup.shape[2]
    per_tick = n_fb // n_chunks
    outs = (q_out, k_out, v_out)
    scale = np.float32(hd ** -0.5)
    below = lax.rem(me + n - 2, n)
    above = lax.rem(me + 2, n)

    await_barrier = entry_barrier(n, me)

    def chunk_rows(i):
        return pl.ds(pl.multiple_of(i * rows, rows), rows)

    def chunk(i):
        return pl.ds(i * PC, PC)

    def tokens_of(s):
        return pl.ds(pl.multiple_of(s * tok, tok), tok)

    def await_bytes(ref, sem):
        pltpu.make_async_copy(ref, ref, sem).wait()

    def x_copy(i):
        return pltpu.make_async_copy(hid.at[chunk(i)], m_buf.at[chunk(i)], x_sem.at[i])

    def head_at(j):
        return lax.rem(2 * chip - n_far + j + n, n)

    def w_copy(j):
        cols = pl.ds(pl.multiple_of(head_at(j) * wide, 128), wide)
        return pltpu.make_async_copy(wqkv.at[:, cols], w_sc.at[j], w_sem.at[j])

    def up_copy(j, slot):
        return pltpu.make_async_copy(wup.at[:, pl.ds(pl.multiple_of(j * fb, 128), fb)], wup_b.at[slot], up_sem.at[slot])

    def dn_copy(j, slot):
        return pltpu.make_async_copy(wdn.at[pl.ds(pl.multiple_of(j * fb, 128), fb)], wdn_b.at[slot], dn_sem.at[slot])

    @pl.loop(0, n_chunks)
    def _(i):
        x_copy(i).start()

    @pl.loop(0, n_w)
    def _(j):
        w_copy(j).start()

    for j in range(2):
        up_copy(j, j).start()
        dn_copy(j, j).start()

    def a_copy(side, i):
        return pltpu.make_async_remote_copy(
            src_ref=a_own.at[chunk_rows(i)], dst_ref=a_nb.at[side, chunk_rows(i)], send_sem=a_send.at[side, i],
            recv_sem=a_recv.at[side, i], device_id={'sp': above if side == 0 else below}, device_id_type=MESH)

    def norm_chunk(i):
        x_copy(i).wait()
        x = m_buf[chunk(i)].reshape(rows, d_model).astype(jnp.float32)
        cen = x - jnp.mean(x, axis=-1, keepdims=True)
        var = jnp.mean(cen * cen, axis=-1, keepdims=True)
        nor = cen * lax.rsqrt(var + LN_EPS)
        a_own[chunk_rows(i)] = (nor * g1[...] + s1[...]).astype(jnp.bfloat16)
        m_buf[chunk(i)] = (nor * g2[...] + s2[...]).astype(jnp.bfloat16).reshape(PC, tok, d_model)
        acc[chunk_rows(i)] = x + (bout[...] + bdn[...])

    norm_chunk(0)
    await_barrier()
    for side in range(2):
        a_copy(side, 0).start()

    @pl.loop(1, n_chunks)
    def _(i):
        norm_chunk(i)

        @pl.when(i < AHEAD)
        def _():
            for side in range(2):
                a_copy(side, i).start()

    @pl.loop(0, n_w)
    def _(j):
        w_copy(j).wait()

    def finish_block(y, head, src, slot, blk):
        t = tokens_of(src)
        cc, cl, cr = tab_c[t][None], tab_l[t][None], tab_r[t][None]
        for m in range(3):
            u = y[:, m * hd:(m + 1) * hd] + bqkv[m, pl.ds(head, 1)]
            if m < 2:
                far = pltpu.roll(u, hd - hd // 8, 1).reshape(PC, tok, hd)
                near = pltpu.roll(u, hd // 8, 1).reshape(PC, tok, hd)
                u = u.reshape(PC, tok, hd) * cc + far * cl + near * cr
            else:
                u = u.reshape(PC, tok, hd)
            st[slot, blk, m] = u.astype(jnp.bfloat16)

    def place(m, i, src):
        return outs[m].at[chunk(i), 0, tokens_of(src)]

    def send_block(i, src, slot, blk, dest):
        for m in range(3):
            pltpu.make_async_remote_copy(
                src_ref=st.at[slot, blk, m], dst_ref=place(m, i, src), send_sem=st_sem.at[slot], recv_sem=r_sem.at[m, i],
                device_id={'sp': dest}, device_id_type=MESH).start()

    def free_slot(slot):
        await_bytes(st.at[slot, pl.ds(0, n_remote)], st_sem.at[slot])
        await_bytes(st.at[slot, pl.ds(0, 3)], self_sem.at[slot])

    def project_chunk(i):
        slot = lax.rem(i, 2)
        r = chunk_rows(i)

        for side in range(2):
            a_copy(side, i).wait_recv()

        @pl.loop(0, n_far)
        def _(t):
            jl = n_w - 1 - t
            y = jnp.dot(a_nb[0, r], w_sc[jl], preferred_element_type=jnp.float32)
            finish_block(y, head_at(jl), below, slot, t)
            send_block(i, below, slot, t, head_at(jl))
            y = jnp.dot(a_nb[1, r], w_sc[t], preferred_element_type=jnp.float32)
            finish_block(y, head_at(t), above, slot, n_far + t)
            send_block(i, above, slot, n_far + t, head_at(t))

        @pl.loop(0, 2)
        def _(q):
            dest = 2 * chip + jnp.where(q == 1, lax.rem(me, 2), 1 - lax.rem(me, 2))
            j = dest - 2 * chip + n_far
            for g, src in enumerate((below, me, above)):
                rows_in = a_own[r] if g == 1 else a_nb[g // 2, r]
                y = jnp.dot(rows_in, w_sc[j], preferred_element_type=jnp.float32)
                finish_block(y, dest, src, slot, 2 * n_far + 3 * q + g)

            @pl.when(q == 0)
            def _():
                for g, src in enumerate((below, me, above)):
                    send_block(i, src, slot, 2 * n_far + g, dest)

            @pl.when(q == 1)
            def _():
                for g, src in enumerate((below, me, above)):
                    for m in range(3):
                        pltpu.make_async_copy(st.at[slot, n_remote + g, m], place(m, i, src), self_sem.at[slot]).start()

    def mlp_block(j):
        slot = lax.rem(j, 2)
        up_copy(j, slot).wait()
        dn_copy(j, slot).wait()
        mp = 2 * PC

        @pl.loop(0, n_prompts // mp)
        def _(r):
            rr = pl.ds(pl.multiple_of(r * mp * tok, mp * tok), mp * tok)
            x = m_buf[pl.ds(r * mp, mp)].reshape(mp * tok, d_model)
            pre = jnp.dot(x, wup_b[slot], preferred_element_type=jnp.float32) + bup[j]
            act = (0.5 * pre * (1.0 + lax.erf(pre * np.float32(np.sqrt(0.5))))).astype(jnp.bfloat16)
            acc[rr] += jnp.dot(act, wdn_b[slot], preferred_element_type=jnp.float32)

        @pl.when(j + 2 < n_fb)
        def _():
            up_copy(j + 2, slot).start()
            dn_copy(j + 2, slot).start()

    blk = seq // 2

    def attend_chunk(i):
        slot = lax.rem(i, 2)
        loads = []
        for m, dst in enumerate((qb, kb, vb)):
            await_bytes(outs[m].at[chunk(0), 0, pl.ds(0, (n - 3) * tok)], r_sem.at[m, i])
            loads.append(pltpu.make_async_copy(outs[m].at[chunk(i), 0], dst, in_sem.at[m]))
            loads[-1].start()

        @pl.when(i >= 2)
        def _():
            await_bytes(ctx_st.at[slot, :, pl.ds(0, (n - 1) * tok)], c_send.at[slot])

        for c in loads:
            c.wait()

        @pl.loop(0, PC)
        def _(p):
            length = lens[i * PC + p]
            for b in range(2):
                keys = (b + 1) * blk
                s = lax.dot_general(qb[p, b * blk:keys], kb[p, :keys], (((1,), (1,)), ((), ())),
                                    preferred_element_type=jnp.float32) * scale
                key = lax.broadcasted_iota(jnp.int32, (blk, keys), 1)
                row = lax.broadcasted_iota(jnp.int32, (blk, keys), 0) + b * blk
                s = jnp.where((key <= row) & (key < length), s, -jnp.inf)
                w = jnp.exp(s - jnp.max(s, axis=-1, keepdims=True))
                z = jnp.sum(w, axis=-1, keepdims=True)
                c = jnp.dot(w.astype(jnp.bfloat16), vb[p, :keys], preferred_element_type=jnp.float32) / z
                ctx_st[slot, p, b * blk:keys] = c.astype(jnp.bfloat16)

        for d in range(1, n):
            dest = lax.rem(me + d, n)
            pltpu.make_async_remote_copy(
                src_ref=ctx_st.at[slot, :, tokens_of(dest)], dst_ref=ctx_rv.at[me, chunk(i)], send_sem=c_send.at[slot],
                recv_sem=c_recv.at[i], device_id={'sp': dest}, device_id_type=MESH).start()
        ctx_rv[me, chunk(i)] = ctx_st[slot, :, tokens_of(me)]

    half = wout.shape[0] // 2
    wo_copies = [pltpu.make_async_copy(wout.at[pl.ds(k * half, half)], a_nb.at[k, pl.ds(0, half)], wo_sem.at[k]) for k in range(2)]

    def store(i, slot):
        return pltpu.make_async_copy(out_b.at[slot], out.at[chunk(i)], o_sem.at[slot])

    def finish_chunk(i):
        slot = lax.rem(i, 2)
        await_bytes(ctx_rv.at[pl.ds(0, n - 1), chunk(0)], c_recv.at[i])

        @pl.when(i >= 2)
        def _():
            store(i - 2, slot).wait()

        width = d_model // 4
        ctx = [jnp.concatenate([ctx_rv[k * (n // 2) + h, chunk(i)].reshape(rows, hd) for h in range(n // 2)], axis=1) for k in range(2)]
        for t in range(4):
            cols = slice(t * width, (t + 1) * width)
            y = acc[chunk_rows(i), cols]
            for k in range(2):
                y = y + jnp.dot(ctx[k], a_nb[k, :half, cols], preferred_element_type=jnp.float32)
            out_b[slot, :, :, cols] = y.astype(jnp.bfloat16).reshape(PC, tok, width)
        store(i, slot).start()

    @pl.loop(0, n_chunks + 2)
    def _(i):
        @pl.when(i + AHEAD < n_chunks)
        def _():
            for side in range(2):
                a_copy(side, i + AHEAD).start()

        @pl.when(i >= 2)
        def _():
            free_slot(lax.rem(i, 2))

        @pl.when(i < n_chunks)
        def _():
            project_chunk(i)

            @pl.when(i == n_chunks - 1)
            def _():
                for c in wo_copies:
                    c.start()

            @pl.loop(0, per_tick)
            def _(j):
                mlp_block(i * per_tick + j)

        @pl.when(i >= 2)
        def _():
            attend_chunk(i - 2)

        @pl.when(i == n_chunks)
        def _():
            for c in wo_copies:
                c.wait()

            @pl.loop(0, n_chunks - 3)
            def _(j):
                finish_chunk(j)

    @pl.loop(n_chunks - 3, n_chunks)
    def _(j):
        finish_chunk(j)

    for slot in range(2):
        await_bytes(ctx_st.at[slot, :, pl.ds(0, (n - 1) * tok)], c_send.at[slot])
        store(n_chunks - 2 + slot, (n_chunks + slot) % 2).wait()

    @pl.loop(0, n_chunks)
    def _(i):
        for side in range(2):
            a_copy(side, i).wait_send()


def hand_on_kernel(a, b, c, a_out, b_out, c_out, a_v, b_v, c_v, in_sem, out_sem):
    parts = in_sem.shape[1]
    size = a.shape[0] // parts
    trio = ((a, a_v, a_out), (b, b_v, b_out), (c, c_v, c_out))

    def copies(t, p):
        src, mid, dst = trio[t]
        s = pl.ds(p * size, size)
        return (pltpu.make_async_copy(src.at[s], mid.at[s], in_sem.at[t, p]),
                pltpu.make_async_copy(mid.at[s], dst.at[s], out_sem.at[t, p]))

    steps = [(t, p) for p in range(parts) for t in range(3)]
    for s in steps:
        copies(*s)[0].start()
    for s in steps:
        copies(*s)[0].wait()
        copies(*s)[1].start()
    for s in steps:
        copies(*s)[1].wait()


def solution(mesh):
    n = mesh.shape['sp']
    row_spec = P('dp', 'sp', None)
    cache_spec = P('dp', 'sp', None, None)
    vec_spec = P(None)
    mat_spec = P(None, None)

    def local_layer(hidden, seq_lens, ln1_gain, ln1_bias, ln2_gain, ln2_bias, w_qkv, b_qkv, w_out, b_out, w_up, b_up, w_down, b_down):
        n_prompts, tok, d_model = hidden.shape
        hd = b_qkv.shape[2]
        d_ff = w_up.shape[1]
        seq = tok * n
        n_rows = n_prompts * tok
        n_chunks = n_prompts // PC
        fb = min(FB, d_ff // n_chunks)
        n_far = n // 2 - 3
        bf, f32 = jnp.bfloat16, jnp.float32
        row = lambda v: v.reshape(1, d_model)
        tabs = [jnp.asarray(t) for t in rotary_tables(seq, hd)]
        cache = jax.ShapeDtypeStruct((n_prompts, 1, seq, hd), bf)
        like_out = jax.ShapeDtypeStruct((n_prompts, tok, d_model), bf)
        dma = pltpu.SemaphoreType.DMA
        q, k, v, out = pl.pallas_call(
            functools.partial(layer_kernel, n),
            name='layer',
            out_shape=(cache, cache, cache, like_out),
            in_specs=[SM, ANY, VM, VM, VM, VM, ANY, VM, VM, VM, VM, ANY, VM, ANY, VM, ANY, VM],
            out_specs=(ANY, ANY, ANY, ANY),
            scratch_shapes=[
                pltpu.VMEM((n_rows, d_model), bf),
                pltpu.VMEM((2, max(n_rows, w_out.shape[0] // 2), d_model), bf),
                pltpu.VMEM((n_prompts, tok, d_model), bf),
                pltpu.VMEM((n_rows, d_model), f32),
                pltpu.VMEM((2 * n_far + 2, d_model, 3 * hd), bf),
                pltpu.VMEM((2, d_model, fb), bf),
                pltpu.VMEM((2, fb, d_model), bf),
                pltpu.VMEM((2, 2 * n_far + 6, 3, PC, tok, hd), bf),
                pltpu.VMEM((PC, seq, hd), bf), pltpu.VMEM((PC, seq, hd), bf), pltpu.VMEM((PC, seq, hd), bf),
                pltpu.VMEM((2, PC, seq, hd), bf),
                pltpu.VMEM((n, n_prompts, tok, hd), bf),
                pltpu.VMEM((2, PC, tok, d_model), bf),
                dma((n_chunks,)), dma((2 * n_far + 2,)), dma((2,)), dma((2,)), dma((2, n_chunks)), dma((2, n_chunks)),
                dma((2,)), dma((2,)), dma((3, n_chunks)), dma((3,)), dma((2,)), dma((n_chunks,)), dma((2,)), dma((2,)),
            ],
            compiler_params=pltpu.CompilerParams(collective_id=0, has_side_effects=True, vmem_limit_bytes=VMEM_LIMIT),
            cost_estimate=pl.CostEstimate(flops=2 * n_rows * d_model * (4 * d_model + 2 * d_ff), bytes_accessed=200_000_000, transcendentals=0),
        )(seq_lens, hidden, row(ln1_gain), row(ln1_bias), row(ln2_gain), row(ln2_bias), w_qkv, jnp.transpose(b_qkv, (1, 0, 2)), *tabs,
          w_up, b_up.reshape(d_ff // fb, 1, fb), w_down, row(b_down), w_out, row(b_out))
        parts = 4
        return pl.pallas_call(
            hand_on_kernel,
            name='hand_on',
            out_shape=(like_out, cache, cache),
            in_specs=[ANY] * 3,
            out_specs=(ANY,) * 3,
            scratch_shapes=[pltpu.VMEM(like_out.shape, bf), pltpu.VMEM(cache.shape, bf), pltpu.VMEM(cache.shape, bf),
                            dma((3, parts)), dma((3, parts))],
            compiler_params=pltpu.CompilerParams(vmem_limit_bytes=VMEM_LIMIT),
        )(out, k, v)

    return jax.shard_map(local_layer, mesh=mesh,
                         in_specs=(row_spec, P('dp'), vec_spec, vec_spec, vec_spec, vec_spec, mat_spec, P(None, None, None), mat_spec, vec_spec, mat_spec, vec_spec, mat_spec, vec_spec),
                         out_specs=(row_spec, cache_spec, cache_spec), check_vma=False)
```

```python
import functools

import jax
import jax.numpy as jnp
import numpy as np
from jax import lax
from jax.experimental import pallas as pl
from jax.experimental.pallas import tpu as pltpu
from jax.sharding import PartitionSpec as P

LN_EPS = 1e-5
ROT_BASE = 10000.0
PC = 4
AHEAD = 3
FB = 512
W_SLOTS = 4
MESH = pl.DeviceIdType.MESH
VMEM_LIMIT = 54_400_000
ANY = pl.BlockSpec(memory_space=pl.ANY)
VM = pl.BlockSpec(memory_space=pltpu.VMEM)
SM = pl.BlockSpec(memory_space=pltpu.SMEM)


def rotary_tables(seq_len, head_dim):
    rot = head_dim // 4
    half = rot // 2
    inv = np.float32(ROT_BASE) ** (np.float32(-2.0) * np.arange(half, dtype=np.float32) / np.float32(rot))
    ang = np.arange(seq_len, dtype=np.float32)[:, None] * inv[None, :].astype(np.float32)
    cos, sin = np.cos(ang), np.sin(ang)
    c = np.ones((seq_len, head_dim), np.float32)
    s = np.zeros((2, seq_len, head_dim), np.float32)
    c[:, :half] = cos
    c[:, half:rot] = cos
    s[0, :, :half] = -sin
    s[1, :, half:rot] = sin
    return c, s[0], s[1]


def entry_barrier(n, me):
    sem = pltpu.get_barrier_semaphore()
    for d in range(1, n):
        pl.semaphore_signal(sem, inc=1, device_id={'sp': lax.rem(me + d, n)}, device_id_type=MESH)
    return lambda: pl.semaphore_wait(sem, n - 1)


def layer_kernel(n, lens, hid, g1, s1, g2, s2, wqkv, bqkv, tab_c, tab_l, tab_r, wup, bup, wdn, bdn, wout, bout,
                 q_out, k_out, v_out, out,
                 a_own, a_nb, m_buf, acc, w_sc, wup_b, wdn_b, st, qb, ctx_st, ctx_rv,
                 x_sem, w_sem, up_sem, dn_sem, a_send, a_recv, st_sem, self_sem, r_sem, in_sem, c_send, c_recv, wo_sem):
    me = lax.axis_index('sp')
    chip = lax.div(me, 2)
    n_prompts, tok, d_model = hid.shape
    seq, hd = q_out.shape[2], q_out.shape[3]
    wide = 3 * hd
    n_chunks = n_prompts // PC
    rows = PC * tok
    n_far = n // 2 - 3
    n_w = 2 * n_far + 2
    n_slots = w_sc.shape[0]
    n_remote = 2 * n_far + 3
    n_fb, fb = bup.shape[0], bup.shape[2]
    per_tick = n_fb // n_chunks
    outs = (q_out, k_out, v_out)
    scale = np.float32(hd ** -0.5)
    below = lax.rem(me + n - 2, n)
    above = lax.rem(me + 2, n)

    await_barrier = entry_barrier(n, me)

    def chunk_rows(i):
        return pl.ds(pl.multiple_of(i * rows, rows), rows)

    def chunk(i):
        return pl.ds(i * PC, PC)

    def tokens_of(s):
        return pl.ds(pl.multiple_of(s * tok, tok), tok)

    def await_bytes(ref, sem):
        pltpu.make_async_copy(ref, ref, sem).wait()

    def x_copy(i):
        return pltpu.make_async_copy(hid.at[chunk(i)], m_buf.at[chunk(i)], x_sem.at[i])

    def head_at(j):
        return lax.rem(2 * chip - n_far + j + n, n)

    def w_copy(k):
        j = jnp.where(k < 2 * n_far, jnp.where(lax.rem(k, 2) == 0, n_w - 1 - lax.div(k, 2), lax.div(k, 2)),
                      n_far + jnp.where(k == 2 * n_far, 1 - lax.rem(me, 2), lax.rem(me, 2)))
        cols = pl.ds(pl.multiple_of(head_at(j) * wide, 128), wide)
        slot = lax.rem(k, n_slots)
        return pltpu.make_async_copy(wqkv.at[:, cols], w_sc.at[slot], w_sem.at[slot])

    def next_weights(i, k):
        after = k + n_slots

        @pl.when((after < n_w) | (i < n_chunks - 1))
        def _():
            w_copy(lax.rem(after, n_w)).start()

    def up_copy(j, slot):
        return pltpu.make_async_copy(wup.at[:, pl.ds(pl.multiple_of(j * fb, 128), fb)], wup_b.at[slot], up_sem.at[slot])

    def dn_copy(j, slot):
        return pltpu.make_async_copy(wdn.at[pl.ds(pl.multiple_of(j * fb, 128), fb)], wdn_b.at[slot], dn_sem.at[slot])

    @pl.loop(0, n_chunks)
    def _(i):
        x_copy(i).start()

    @pl.loop(0, n_slots)
    def _(k):
        w_copy(k).start()

    for j in range(2):
        up_copy(j, j).start()
        dn_copy(j, j).start()

    def a_copy(side, i):
        return pltpu.make_async_remote_copy(
            src_ref=a_own.at[chunk_rows(i)], dst_ref=a_nb.at[side, chunk_rows(i)], send_sem=a_send.at[side, i],
            recv_sem=a_recv.at[side, i], device_id={'sp': above if side == 0 else below}, device_id_type=MESH)

    def norm_chunk(i):
        x_copy(i).wait()
        x = m_buf[chunk(i)].reshape(rows, d_model).astype(jnp.float32)
        cen = x - jnp.mean(x, axis=-1, keepdims=True)
        var = jnp.mean(cen * cen, axis=-1, keepdims=True)
        nor = cen * lax.rsqrt(var + LN_EPS)
        a_own[chunk_rows(i)] = (nor * g1[...] + s1[...]).astype(jnp.bfloat16)
        m_buf[chunk(i)] = (nor * g2[...] + s2[...]).astype(jnp.bfloat16).reshape(PC, tok, d_model)
        acc[chunk_rows(i)] = x + (bout[...] + bdn[...])

    norm_chunk(0)
    await_barrier()
    for side in range(2):
        a_copy(side, 0).start()

    @pl.loop(1, n_chunks)
    def _(i):
        norm_chunk(i)

        @pl.when(i < AHEAD)
        def _():
            for side in range(2):
                a_copy(side, i).start()

    def finish_block(y, head, src, slot, blk):
        t = tokens_of(src)
        cc, cl, cr = tab_c[t][None], tab_l[t][None], tab_r[t][None]
        for m in range(3):
            u = y[:, m * hd:(m + 1) * hd] + bqkv[m, pl.ds(head, 1)]
            if m < 2:
                far = pltpu.roll(u, hd - hd // 8, 1).reshape(PC, tok, hd)
                near = pltpu.roll(u, hd // 8, 1).reshape(PC, tok, hd)
                u = u.reshape(PC, tok, hd) * cc + far * cl + near * cr
            else:
                u = u.reshape(PC, tok, hd)
            st[slot, blk, m] = u.astype(jnp.bfloat16)

    def place(m, i, src):
        return outs[m].at[chunk(i), 0, tokens_of(src)]

    def send_block(i, src, slot, blk, dest):
        for m in range(3):
            pltpu.make_async_remote_copy(
                src_ref=st.at[slot, blk, m], dst_ref=place(m, i, src), send_sem=st_sem.at[slot], recv_sem=r_sem.at[m, i],
                device_id={'sp': dest}, device_id_type=MESH).start()

    def free_slot(slot):
        await_bytes(st.at[slot, pl.ds(0, n_remote)], st_sem.at[slot])
        await_bytes(st.at[slot, pl.ds(0, 3)], self_sem.at[slot])

    def project_chunk(i):
        slot = lax.rem(i, 2)
        r = chunk_rows(i)

        for side in range(2):
            a_copy(side, i).wait_recv()

        @pl.loop(0, n_far)
        def _(t):
            for side, (src, j) in enumerate(((below, n_w - 1 - t), (above, t))):
                k = 2 * t + side
                w_copy(k).wait()
                y = jnp.dot(a_nb[side, r], w_sc[lax.rem(k, n_slots)], preferred_element_type=jnp.float32)
                finish_block(y, head_at(j), src, slot, side * n_far + t)
                send_block(i, src, slot, side * n_far + t, head_at(j))
                next_weights(i, k)

        @pl.loop(0, 2)
        def _(q):
            dest = 2 * chip + jnp.where(q == 1, lax.rem(me, 2), 1 - lax.rem(me, 2))
            k = 2 * n_far + q
            w_copy(k).wait()
            for g, src in enumerate((below, me, above)):
                rows_in = a_own[r] if g == 1 else a_nb[g // 2, r]
                y = jnp.dot(rows_in, w_sc[lax.rem(k, n_slots)], preferred_element_type=jnp.float32)
                finish_block(y, dest, src, slot, 2 * n_far + 3 * q + g)
            next_weights(i, k)

            @pl.when(q == 0)
            def _():
                for g, src in enumerate((below, me, above)):
                    send_block(i, src, slot, 2 * n_far + g, dest)

            @pl.when(q == 1)
            def _():
                for g, src in enumerate((below, me, above)):
                    for m in range(3):
                        pltpu.make_async_copy(st.at[slot, n_remote + g, m], place(m, i, src), self_sem.at[slot]).start()

    def mlp_block(j):
        slot = lax.rem(j, 2)
        up_copy(j, slot).wait()
        dn_copy(j, slot).wait()
        mp = 2 * PC

        @pl.loop(0, n_prompts // mp)
        def _(r):
            rr = pl.ds(pl.multiple_of(r * mp * tok, mp * tok), mp * tok)
            x = m_buf[pl.ds(r * mp, mp)].reshape(mp * tok, d_model)
            pre = jnp.dot(x, wup_b[slot], preferred_element_type=jnp.float32) + bup[j]
            act = (0.5 * pre * (1.0 + lax.erf(pre * np.float32(np.sqrt(0.5))))).astype(jnp.bfloat16)
            acc[rr] += jnp.dot(act, wdn_b[slot], preferred_element_type=jnp.float32)

        @pl.when(j + 2 < n_fb)
        def _():
            up_copy(j + 2, slot).start()
            dn_copy(j + 2, slot).start()

    blk = seq // 2

    def attend_chunk(i):
        slot = lax.rem(i, 2)
        for m in range(3):
            await_bytes(outs[m].at[chunk(0), 0, pl.ds(0, (n - 3) * tok)], r_sem.at[m, i])
        q_load = pltpu.make_async_copy(q_out.at[chunk(i), 0], qb, in_sem)
        q_load.start()

        @pl.when(i >= 2)
        def _():
            await_bytes(ctx_st.at[slot, :, pl.ds(0, (n - 1) * tok)], c_send.at[slot])

        q_load.wait()

        @pl.loop(0, PC)
        def _(p):
            length = lens[i * PC + p]
            for b in range(2):
                keys = (b + 1) * blk
                s = lax.dot_general(qb[p, b * blk:keys], k_out[i * PC + p, 0, :keys], (((1,), (1,)), ((), ())),
                                    preferred_element_type=jnp.float32) * scale
                key = lax.broadcasted_iota(jnp.int32, (blk, keys), 1)
                row = lax.broadcasted_iota(jnp.int32, (blk, keys), 0) + b * blk
                s = jnp.where((key <= row) & (key < length), s, -jnp.inf)
                w = jnp.exp(s - jnp.max(s, axis=-1, keepdims=True))
                z = jnp.sum(w, axis=-1, keepdims=True)
                c = jnp.dot(w.astype(jnp.bfloat16), v_out[i * PC + p, 0, :keys], preferred_element_type=jnp.float32) / z
                ctx_st[slot, p, b * blk:keys] = c.astype(jnp.bfloat16)

        for d in range(1, n):
            dest = lax.rem(me + d, n)
            pltpu.make_async_remote_copy(
                src_ref=ctx_st.at[slot, :, tokens_of(dest)], dst_ref=ctx_rv.at[me, chunk(i)], send_sem=c_send.at[slot],
                recv_sem=c_recv.at[i], device_id={'sp': dest}, device_id_type=MESH).start()
        ctx_rv[me, chunk(i)] = ctx_st[slot, :, tokens_of(me)]

    half = wout.shape[0] // 2
    wo_copies = [pltpu.make_async_copy(wout.at[pl.ds(k * half, half)], a_nb.at[k, pl.ds(0, half)], wo_sem.at[k]) for k in range(2)]

    def finish_chunk(i):
        await_bytes(ctx_rv.at[pl.ds(0, n - 1), chunk(0)], c_recv.at[i])
        width = d_model // 4
        ctx = [jnp.concatenate([ctx_rv[k * (n // 2) + h, chunk(i)].reshape(rows, hd) for h in range(n // 2)], axis=1) for k in range(2)]
        for t in range(4):
            cols = slice(t * width, (t + 1) * width)
            y = acc[chunk_rows(i), cols]
            for k in range(2):
                y = y + jnp.dot(ctx[k], a_nb[k, :half, cols], preferred_element_type=jnp.float32)
            out[chunk(i), :, cols] = y.astype(jnp.bfloat16).reshape(PC, tok, width)

    @pl.loop(0, n_chunks + 2)
    def _(i):
        @pl.when(i + AHEAD < n_chunks)
        def _():
            for side in range(2):
                a_copy(side, i + AHEAD).start()

        @pl.when(i >= 2)
        def _():
            free_slot(lax.rem(i, 2))

        @pl.when(i < n_chunks)
        def _():
            project_chunk(i)

            @pl.when(i == n_chunks - 1)
            def _():
                for c in wo_copies:
                    c.start()

            @pl.loop(0, per_tick)
            def _(j):
                mlp_block(i * per_tick + j)

        @pl.when(i >= 2)
        def _():
            attend_chunk(i - 2)

        @pl.when(i == n_chunks)
        def _():
            for c in wo_copies:
                c.wait()

            @pl.loop(0, n_chunks - 3)
            def _(j):
                finish_chunk(j)

    @pl.loop(n_chunks - 3, n_chunks)
    def _(j):
        finish_chunk(j)

    for slot in range(2):
        await_bytes(ctx_st.at[slot, :, pl.ds(0, (n - 1) * tok)], c_send.at[slot])

    @pl.loop(0, n_chunks)
    def _(i):
        for side in range(2):
            a_copy(side, i).wait_send()


def hand_on_kernel(a, b, c, a_out, b_out, c_out, sem):
    parts = sem.shape[1]
    size = a.shape[0] // parts
    copies = [pltpu.make_async_copy(src.at[pl.ds(p * size, size)], dst.at[pl.ds(p * size, size)], sem.at[t, p])
              for p in range(parts) for t, (src, dst) in enumerate(((a, a_out), (b, b_out), (c, c_out)))]
    for copy in copies:
        copy.start()
    for copy in copies:
        copy.wait()


def solution(mesh):
    n = mesh.shape['sp']
    row_spec = P('dp', 'sp', None)
    cache_spec = P('dp', 'sp', None, None)
    vec_spec = P(None)
    mat_spec = P(None, None)

    def local_layer(hidden, seq_lens, ln1_gain, ln1_bias, ln2_gain, ln2_bias, w_qkv, b_qkv, w_out, b_out, w_up, b_up, w_down, b_down):
        n_prompts, tok, d_model = hidden.shape
        hd = b_qkv.shape[2]
        d_ff = w_up.shape[1]
        seq = tok * n
        n_rows = n_prompts * tok
        n_chunks = n_prompts // PC
        fb = min(FB, d_ff // n_chunks)
        n_far = n // 2 - 3
        bf, f32 = jnp.bfloat16, jnp.float32
        row = lambda v: v.reshape(1, d_model)
        tabs = [jnp.asarray(t) for t in rotary_tables(seq, hd)]
        cache = jax.ShapeDtypeStruct((n_prompts, 1, seq, hd), bf)
        like_out = jax.ShapeDtypeStruct((n_prompts, tok, d_model), bf)
        dma = pltpu.SemaphoreType.DMA
        q, k, v, out = pl.pallas_call(
            functools.partial(layer_kernel, n),
            name='layer',
            out_shape=(cache, pltpu.VMEM(cache.shape, bf), pltpu.VMEM(cache.shape, bf), pltpu.VMEM(like_out.shape, bf)),
            in_specs=[SM, ANY, VM, VM, VM, VM, ANY, VM, VM, VM, VM, ANY, VM, ANY, VM, ANY, VM],
            out_specs=(ANY, VM, VM, VM),
            scratch_shapes=[
                pltpu.VMEM((n_rows, d_model), bf),
                pltpu.VMEM((2, max(n_rows, w_out.shape[0] // 2), d_model), bf),
                pltpu.VMEM((n_prompts, tok, d_model), bf),
                pltpu.VMEM((n_rows, d_model), f32),
                pltpu.VMEM((W_SLOTS, d_model, 3 * hd), bf),
                pltpu.VMEM((2, d_model, fb), bf),
                pltpu.VMEM((2, fb, d_model), bf),
                pltpu.VMEM((2, 2 * n_far + 6, 3, PC, tok, hd), bf),
                pltpu.VMEM((PC, seq, hd), bf),
                pltpu.VMEM((2, PC, seq, hd), bf),
                pltpu.VMEM((n, n_prompts, tok, hd), bf),
                dma((n_chunks,)), dma((W_SLOTS,)), dma((2,)), dma((2,)), dma((2, n_chunks)), dma((2, n_chunks)),
                dma((2,)), dma((2,)), dma((3, n_chunks)), dma(()), dma((2,)), dma((n_chunks,)), dma((2,)),
            ],
            compiler_params=pltpu.CompilerParams(collective_id=0, has_side_effects=True, vmem_limit_bytes=VMEM_LIMIT),
            cost_estimate=pl.CostEstimate(flops=2 * n_rows * d_model * (4 * d_model + 2 * d_ff), bytes_accessed=200_000_000, transcendentals=0),
        )(seq_lens, hidden, row(ln1_gain), row(ln1_bias), row(ln2_gain), row(ln2_bias), w_qkv, jnp.transpose(b_qkv, (1, 0, 2)), *tabs,
          w_up, b_up.reshape(d_ff // fb, 1, fb), w_down, row(b_down), w_out, row(b_out))
        parts = 4
        return pl.pallas_call(
            hand_on_kernel,
            name='hand_on',
            out_shape=(like_out, cache, cache),
            in_specs=[VM] * 3,
            out_specs=(ANY,) * 3,
            scratch_shapes=[dma((3, parts))],
            compiler_params=pltpu.CompilerParams(vmem_limit_bytes=1 << 20),
        )(*(pltpu.with_memory_space_constraint(t, pltpu.VMEM) for t in (out, k, v)))

    return jax.shard_map(local_layer, mesh=mesh,
                         in_specs=(row_spec, P('dp'), vec_spec, vec_spec, vec_spec, vec_spec, mat_spec, P(None, None, None), mat_spec, vec_spec, mat_spec, vec_spec, mat_spec, vec_spec),
                         out_specs=(row_spec, cache_spec, cache_spec), check_vma=False)
```

```python
import functools

import jax
import jax.numpy as jnp
import numpy as np
from jax import lax
from jax.experimental import pallas as pl
from jax.experimental.pallas import tpu as pltpu
from jax.sharding import PartitionSpec as P

LN_EPS = 1e-5
ROT_BASE = 10000.0
PC = 4
AHEAD = 3
FB = 512
W_SLOTS = 4
HOME = 2
MESH = pl.DeviceIdType.MESH
VMEM_LIMIT = 54_400_000
ANY = pl.BlockSpec(memory_space=pl.ANY)
VM = pl.BlockSpec(memory_space=pltpu.VMEM)
SM = pl.BlockSpec(memory_space=pltpu.SMEM)


def rotary_tables(seq_len, head_dim):
    rot = head_dim // 4
    half = rot // 2
    inv = np.float32(ROT_BASE) ** (np.float32(-2.0) * np.arange(half, dtype=np.float32) / np.float32(rot))
    ang = np.arange(seq_len, dtype=np.float32)[:, None] * inv[None, :].astype(np.float32)
    cos, sin = np.cos(ang), np.sin(ang)
    c = np.ones((seq_len, head_dim), np.float32)
    s = np.zeros((2, seq_len, head_dim), np.float32)
    c[:, :half] = cos
    c[:, half:rot] = cos
    s[0, :, :half] = -sin
    s[1, :, half:rot] = sin
    return np.stack([c, s[0], s[1]])


def entry_barrier(n, me):
    sem = pltpu.get_barrier_semaphore()
    for d in range(1, n):
        pl.semaphore_signal(sem, inc=1, device_id={'sp': lax.rem(me + d, n)}, device_id_type=MESH)
    return lambda: pl.semaphore_wait(sem, n - 1)


def layer_kernel(n, lens, hid, g1, s1, g2, s2, wqkv, bqkv, tabs, wup, bup, wdn, bdn, wout, bout,
                 q_out, k_out, v_out, out, p_rows,
                 a_own, a_nb, m_buf, acc, w_sc, wup_b, wdn_b, st, qb, ctx_st, ctx_rv, p_buf, hq, hk, hv, h_st, tab,
                 x_sem, w_sem, up_sem, dn_sem, a_send, a_recv, st_sem, self_sem, r_sem, in_sem, c_send, c_recv, wo_sem, p_send, p_recv, p_sem, h_send, t_sem):
    me = lax.axis_index('sp')
    chip = lax.div(me, 2)
    n_prompts, tok, d_model = hid.shape
    seq, hd = q_out.shape[2], q_out.shape[3]
    wide = 3 * hd
    n_chunks = n_prompts // PC
    rows = PC * tok
    n_far = n // 2 - 3
    n_w = 2 * n_far + 2
    n_slots = w_sc.shape[0]
    n_remote = 2 * n_far + 3
    n_fb, fb = bup.shape[0], bup.shape[2]
    per_tick = n_fb // n_chunks
    outs = (q_out, k_out, v_out)
    scale = np.float32(hd ** -0.5)
    below = lax.rem(me + n - 2, n)
    above = lax.rem(me + 2, n)

    core = lax.rem(me, 2)
    partner = me + 1 - 2 * core
    beside = lax.rem(partner + n - 2, n)
    n_home = 2 * HOME
    at_home = me < n_home
    home_tok = n_home * tok
    n_own = n // 2
    n_stay = (below < n_home).astype(jnp.int32) + at_home.astype(jnp.int32) + (above < n_home).astype(jnp.int32)

    def by_stay(do):
        for v in range(3):
            pl.when(n_stay == v)(functools.partial(do, v))

    await_barrier = entry_barrier(n, me)

    def chunk_rows(i):
        return pl.ds(pl.multiple_of(i * rows, rows), rows)

    def chunk(i):
        return pl.ds(i * PC, PC)

    def tokens_of(s):
        return pl.ds(pl.multiple_of(s * tok, tok), tok)

    def await_bytes(ref, sem):
        pltpu.make_async_copy(ref, ref, sem).wait()

    def x_copy(i):
        return pltpu.make_async_copy(hid.at[chunk(i)], m_buf.at[chunk(i)], x_sem.at[i])

    def head_at(j):
        return lax.rem(2 * chip - n_far + j + n, n)

    def w_copy(k):
        j = jnp.where(k < 2 * n_far, jnp.where(lax.rem(k, 2) == 0, n_w - 1 - lax.div(k, 2), lax.div(k, 2)),
                      n_far + jnp.where(k == 2 * n_far, 1 - core, core))
        head = jnp.where(k < n_w, head_at(j), n_own * core + k - n_w)
        cols = pl.ds(pl.multiple_of(head * wide, 128), wide)
        slot = lax.rem(k, n_slots)
        return pltpu.make_async_copy(wqkv.at[:, cols], w_sc.at[slot], w_sem.at[slot])

    last_tick = n_chunks - 1 + jnp.where(at_home, 2, 0)

    def next_weights(i, k):
        after = k + n_slots
        end = jnp.where(at_home & (i >= 2), n_w + n_own, n_w)
        start = jnp.where(i + 1 < n_chunks, 0, n_w)

        @pl.when((after < end) | (i < last_tick))
        def _():
            w_copy(jnp.where(after < end, after, start + after - end)).start()

    def up_copy(j, slot):
        return pltpu.make_async_copy(wup.at[:, pl.ds(pl.multiple_of(j * fb, 128), fb)], wup_b.at[slot], up_sem.at[slot])

    def dn_copy(j, slot):
        return pltpu.make_async_copy(wdn.at[pl.ds(pl.multiple_of(j * fb, 128), fb)], wdn_b.at[slot], dn_sem.at[slot])

    sources = (below, me, above, beside, partner)
    tab_copies = [pltpu.make_async_copy(tabs.at[:, tokens_of(src)], tab.at[g], t_sem.at[g]) for g, src in enumerate(sources)]

    @pl.loop(0, n_chunks)
    def _(i):
        x_copy(i).start()

    @pl.loop(0, n_slots)
    def _(k):
        w_copy(k).start()

    for c in tab_copies:
        c.start()

    for j in range(2):
        up_copy(j, j).start()
        dn_copy(j, j).start()

    def a_copy(side, i):
        return pltpu.make_async_remote_copy(
            src_ref=a_own.at[chunk_rows(i)], dst_ref=a_nb.at[side, chunk_rows(i)], send_sem=a_send.at[side, i],
            recv_sem=a_recv.at[side, i], device_id={'sp': above if side == 0 else below}, device_id_type=MESH)

    def norm_chunk(i):
        x_copy(i).wait()

        @pl.loop(0, PC)
        def _(p):
            b = i * PC + p
            r = pl.ds(pl.multiple_of(b * tok, tok), tok)
            x = m_buf[b].astype(jnp.float32)
            cen = x - jnp.mean(x, axis=-1, keepdims=True)
            var = jnp.mean(cen * cen, axis=-1, keepdims=True)
            nor = cen * lax.rsqrt(var + LN_EPS)
            a_own[r] = (nor * g1[...] + s1[...]).astype(jnp.bfloat16)
            m_buf[b] = (nor * g2[...] + s2[...]).astype(jnp.bfloat16)
            acc[r] = x + (bout[...] + bdn[...])

    norm_chunk(0)
    await_barrier()
    for side in range(2):
        a_copy(side, 0).start()

    @pl.loop(1, n_chunks)
    def _(i):
        norm_chunk(i)

        @pl.when(i < AHEAD)
        def _():
            for side in range(2):
                a_copy(side, i).start()

    def finish_block(y, head, g, put, parts=(0, 1, 2)):
        cc, cl, cr = (tab[g, t][None] for t in range(3))
        for m in parts:
            u = y[:, (m - parts[0]) * hd:(m - parts[0] + 1) * hd] + bqkv[m, pl.ds(head, 1)]
            if m < 2:
                far = pltpu.roll(u, hd - hd // 8, 1).reshape(PC, tok, hd)
                near = pltpu.roll(u, hd // 8, 1).reshape(PC, tok, hd)
                u = u.reshape(PC, tok, hd) * cc + far * cl + near * cr
            else:
                u = u.reshape(PC, tok, hd)
            put(m, u.astype(jnp.bfloat16))

    def stage(slot, blk):
        def put(m, u):
            st[slot, blk, m] = u
        return put

    def place(m, i, src):
        return outs[m].at[chunk(i), 0, tokens_of(src)]

    def send_block(i, src, slot, blk, dest):
        def send(m):
            pltpu.make_async_remote_copy(
                src_ref=st.at[slot, blk, m], dst_ref=place(m, i, src), send_sem=st_sem.at[slot, min(m, 1)],
                recv_sem=r_sem.at[m, i], device_id={'sp': dest}, device_id_type=MESH).start()
        pl.when(src >= n_home)(lambda: send(0))
        send(1)
        send(2)

    def free_slot(slot):
        await_bytes(st.at[slot, pl.ds(0, n_remote), pl.ds(0, 2)], st_sem.at[slot, 1])
        await_bytes(st.at[slot, pl.ds(0, 3), pl.ds(0, 2)], self_sem.at[slot, 1])

        def queries(v):
            await_bytes(st.at[slot, pl.ds(0, (n_far if v else 2 * n_far) + 3 - v), 0], st_sem.at[slot, 0])
            await_bytes(st.at[slot, pl.ds(0, 3 - v), 0], self_sem.at[slot, 0])
        by_stay(queries)

    def p_copy(b, i):
        src = a_own.at[chunk_rows(i)] if b == 0 else a_nb.at[0, chunk_rows(i)]
        return pltpu.make_async_remote_copy(
            src_ref=src, dst_ref=p_rows.at[b, chunk_rows(i)], send_sem=p_send.at[b, i], recv_sem=p_recv.at[b, i],
            device_id={'sp': partner}, device_id_type=MESH)

    def project_chunk(i):
        slot = lax.rem(i, 2)
        r = chunk_rows(i)

        for side in range(2):
            a_copy(side, i).wait_recv()

        @pl.when(at_home)
        def _():
            for b in range(2):
                p_copy(b, i).start()

        @pl.loop(0, n_far)
        def _(t):
            ends = ((below, n_w - 1 - t), (above, t))
            for side in range(2):
                w_copy(2 * t + side).wait()
            y = [jnp.dot(a_nb[side, r], w_sc[lax.rem(2 * t + side, n_slots)], preferred_element_type=jnp.float32) for side in range(2)]
            for side, (src, j) in enumerate(ends):
                finish_block(y[side], head_at(j), 2 * side, stage(slot, side * n_far + t))
            for side, (src, j) in enumerate(ends):
                send_block(i, src, slot, side * n_far + t, head_at(j))
            for side in range(2):
                next_weights(i, 2 * t + side)

        @pl.loop(0, 2)
        def _(q):
            dest = 2 * chip + jnp.where(q == 1, core, 1 - core)
            k = 2 * n_far + q
            w_copy(k).wait()
            for g, src in enumerate((below, me, above)):
                rows_in = a_own[r] if g == 1 else a_nb[g // 2, r]
                y = jnp.dot(rows_in, w_sc[lax.rem(k, n_slots)], preferred_element_type=jnp.float32)
                finish_block(y, dest, g, stage(slot, 2 * n_far + 3 * q + g))
            next_weights(i, k)

            @pl.when(q == 0)
            def _():
                for g, src in enumerate((below, me, above)):
                    send_block(i, src, slot, 2 * n_far + g, dest)

            @pl.when(q == 1)
            def _():
                for g, src in enumerate((below, me, above)):
                    def keep(m, g=g, src=src):
                        pltpu.make_async_copy(st.at[slot, n_remote + g, m], place(m, i, src), self_sem.at[slot, min(m, 1)]).start()
                    pl.when(src >= n_home)(functools.partial(keep, 0))
                    keep(1)
                    keep(2)

    def mlp_block(j):
        slot = lax.rem(j, 2)
        up_copy(j, slot).wait()
        dn_copy(j, slot).wait()
        mp = 2 * PC

        @pl.loop(0, n_prompts // mp)
        def _(r):
            rr = pl.ds(pl.multiple_of(r * mp * tok, mp * tok), mp * tok)
            x = m_buf[pl.ds(r * mp, mp)].reshape(mp * tok, d_model)
            pre = jnp.dot(x, wup_b[slot], preferred_element_type=jnp.float32) + bup[j]
            act = (0.5 * pre * (1.0 + lax.erf(pre * np.float32(np.sqrt(0.5))))).astype(jnp.bfloat16)
            acc[rr] += jnp.dot(act, wdn_b[slot], preferred_element_type=jnp.float32)

        @pl.when(j + 2 < n_fb)
        def _():
            up_copy(j + 2, slot).start()
            dn_copy(j + 2, slot).start()

    blk = seq // 2

    def q_load(i):
        return pltpu.make_async_copy(q_out.at[chunk(i), 0, pl.ds(home_tok, seq - home_tok)], qb, in_sem)

    def free_ctx(slot):
        for home in range(2):
            @pl.when(at_home == bool(home))
            def _():
                await_bytes(ctx_st.at[slot, :, pl.ds(0, (n - n_home - 1 + home) * tok)], c_send.at[slot])

    def p_load(b, i):
        return pltpu.make_async_copy(p_rows.at[b, chunk_rows(i)], p_buf.at[b], p_sem.at[b])

    def gather_chunk(i):
        @pl.when(at_home)
        def _():
            for b in range(2):
                p_copy(b, i).wait_recv()
                p_load(b, i).start()

        for m in range(1, 3):
            await_bytes(outs[m].at[chunk(0), 0, pl.ds(0, (n - 3) * tok)], r_sem.at[m, i])
        by_stay(lambda v: await_bytes(q_out.at[chunk(0), 0, pl.ds(0, (n - n_home - 3 + v) * tok)], r_sem.at[0, i]))
        q_load(i).start()

    def attend_chunk(i):
        slot = lax.rem(i, 2)

        @pl.when(i >= 2)
        def _():
            free_ctx(slot)

        q_load(i).wait()

        @pl.loop(0, PC)
        def _(p):
            length = lens[i * PC + p]
            for b in range(2):
                keys = (b + 1) * blk
                first = max(b * blk, home_tok)
                s = lax.dot_general(qb[p, first - home_tok:keys - home_tok], k_out[i * PC + p, 0, :keys], (((1,), (1,)), ((), ())),
                                    preferred_element_type=jnp.float32) * scale
                key = lax.broadcasted_iota(jnp.int32, (keys - first, keys), 1)
                row = lax.broadcasted_iota(jnp.int32, (keys - first, keys), 0) + first
                s = jnp.where((key <= row) & (key < length), s, -jnp.inf)
                w = jnp.exp(s - jnp.max(s, axis=-1, keepdims=True))
                z = jnp.sum(w, axis=-1, keepdims=True)
                c = jnp.dot(w.astype(jnp.bfloat16), v_out[i * PC + p, 0, :keys], preferred_element_type=jnp.float32) / z
                ctx_st[slot, p, first - home_tok:keys - home_tok] = c.astype(jnp.bfloat16)

        for d in range(1, n):
            dest = lax.rem(me + d, n)

            @pl.when(dest >= n_home)
            def _():
                pltpu.make_async_remote_copy(
                    src_ref=ctx_st.at[slot, :, tokens_of(dest - n_home)], dst_ref=ctx_rv.at[me, chunk(i)],
                    send_sem=c_send.at[slot], recv_sem=c_recv.at[i], device_id={'sp': dest}, device_id_type=MESH).start()

        @pl.when(me >= n_home)
        def _():
            ctx_rv[me, chunk(i)] = ctx_st[slot, :, tokens_of(me - n_home)]

    def h_copy(i, slot):
        return pltpu.make_async_remote_copy(
            src_ref=h_st.at[slot], dst_ref=ctx_rv.at[pl.ds(n_own * core, n_own), chunk(i)], send_sem=h_send.at[slot],
            recv_sem=c_recv.at[i], device_id={'sp': partner}, device_id_type=MESH)

    def home_chunk(i):
        slot = lax.rem(i, 2)
        r = chunk_rows(i)
        @pl.when(i >= 2)
        def _():
            h_copy(i - 2, slot).wait_send()

        for b in range(2):
            p_load(b, i).wait()

        kinds = (below, beside, me, partner)

        def positions(shards, shape, dim):
            t = lax.broadcasted_iota(jnp.int32, shape, dim)
            pos = t + shards[0] * tok
            for b in range(1, len(shards)):
                pos = jnp.where(t >= b * tok, t + (shards[b] - b) * tok, pos)
            return pos

        key = positions(kinds, (2 * tok, 4 * tok), 1)
        row = positions(kinds[2:], (2 * tok, 4 * tok), 0)

        def project_head(h):
            w = w_sc.at[lax.rem(n_w + h, n_slots)]
            par = lax.rem(h, 2)
            own = jnp.dot(jnp.concatenate([a_own[r], p_buf[0]], axis=0), w[...], preferred_element_type=jnp.float32)
            old = jnp.dot(jnp.concatenate([a_nb[0, r], p_buf[1]], axis=0), w[:, hd:], preferred_element_type=jnp.float32)
            for b in range(4):
                def put(m, u, b=b):
                    (hq, hk, hv)[m][par, b - 2 if m == 0 else b] = u
                y = (old if b < 2 else own)[b % 2 * rows:(b % 2 + 1) * rows]
                finish_block(y, n_own * core + h, (0, 3, 1, 4)[b], put, (0, 1, 2) if b >= 2 else (1, 2))

        def attend_head(h):
            par = lax.rem(h, 2)
            head = n_own * core + h
            s = [lax.dot_general(hq[par, :, p].reshape(2 * tok, hd), hk[par, :, p].reshape(4 * tok, hd), (((1,), (1,)), ((), ())),
                                 preferred_element_type=jnp.float32) * scale for p in range(PC)]
            s = [jnp.where((key <= row) & (key < lens[i * PC + p]), s[p], -jnp.inf) for p in range(PC)]
            w = [jnp.exp(t - jnp.max(t, axis=-1, keepdims=True)) for t in s]
            z = [jnp.sum(t, axis=-1, keepdims=True) for t in w]
            for p in range(PC):
                c = jnp.dot(w[p].astype(jnp.bfloat16), hv[par, :, p].reshape(4 * tok, hd), preferred_element_type=jnp.float32) / z[p]
                c = c.astype(jnp.bfloat16)
                ctx_rv[head, i * PC + p] = c[:tok]
                h_st[slot, h, p] = c[tok:]

        w_copy(n_w).wait()
        project_head(0)
        next_weights(i + 2, n_w)

        @pl.loop(1, n_own)
        def _(h):
            w_copy(n_w + h).wait()
            attend_head(h - 1)
            project_head(h)
            next_weights(i + 2, n_w + h)
        attend_head(n_own - 1)
        h_copy(i, slot).start()

    for c in tab_copies:
        c.wait()

    n_blk = d_model // fb
    wo_copies = []
    for t in range(n_blk):
        cols = pl.ds(t * fb, fb)
        if t < 2:
            wo_copies.append(pltpu.make_async_copy(wout.at[:, cols], wup_b.at[t], up_sem.at[t]))
        else:
            for k in range(n_blk):
                wo_copies.append(pltpu.make_async_copy(wout.at[pl.ds(k * fb, fb), cols], wdn_b.at[t - 2, :, pl.ds(k * fb, fb)], wo_sem.at[t - 2, k]))

    def finish_chunk(i):
        for home in range(2):
            @pl.when(at_home == bool(home))
            def _():
                await_bytes(ctx_rv.at[pl.ds(0, n_own if home else n - 1), chunk(0)], c_recv.at[i])
        ctx = jnp.concatenate([ctx_rv[h, chunk(i)].reshape(rows, hd) for h in range(n)], axis=1)
        for t in range(n_blk):
            cols = slice(t * fb, (t + 1) * fb)
            y = acc[chunk_rows(i), cols]
            if t < 2:
                y = y + jnp.dot(ctx, wup_b[t], preferred_element_type=jnp.float32)
            else:
                w = jnp.concatenate([wdn_b[t - 2, :, k * fb:(k + 1) * fb] for k in range(n_blk)], axis=0)
                y = y + jnp.dot(ctx, w, preferred_element_type=jnp.float32)
            out[chunk(i), :, cols] = y.astype(jnp.bfloat16).reshape(PC, tok, fb)

    @pl.loop(0, n_chunks + 2)
    def _(i):
        @pl.when(i + AHEAD < n_chunks)
        def _():
            for side in range(2):
                a_copy(side, i + AHEAD).start()

        @pl.when(i >= 2)
        def _():
            free_slot(lax.rem(i, 2))

        @pl.when(i < n_chunks)
        def _():
            project_chunk(i)

        @pl.when(i >= 2)
        def _():
            gather_chunk(i - 2)

        @pl.when(i < n_chunks)
        def _():
            @pl.loop(0, per_tick)
            def _(j):
                mlp_block(i * per_tick + j)

            @pl.when(i == n_chunks - 1)
            def _():
                for c in wo_copies:
                    c.start()

        @pl.when(i >= 2)
        def _():
            attend_chunk(i - 2)

            @pl.when(at_home)
            def _():
                home_chunk(i - 2)

        @pl.when(i == n_chunks)
        def _():
            for c in wo_copies:
                c.wait()

            @pl.loop(0, n_chunks - 3)
            def _(j):
                finish_chunk(j)

    @pl.loop(n_chunks - 3, n_chunks)
    def _(j):
        finish_chunk(j)

    for slot in range(2):
        free_ctx(slot)

        @pl.when(at_home)
        def _():
            h_copy(n_chunks - 2 + slot, (n_chunks + slot) % 2).wait_send()
            for b in range(2):
                @pl.loop(slot, n_chunks, step=2)
                def _(j):
                    p_copy(b, j).wait_send()

    @pl.loop(0, n_chunks)
    def _(i):
        for side in range(2):
            a_copy(side, i).wait_send()


def hand_on_kernel(a, b, c, a_out, b_out, c_out, sem):
    parts = sem.shape[1]
    size = a.shape[0] // parts
    copies = [pltpu.make_async_copy(src.at[pl.ds(p * size, size)], dst.at[pl.ds(p * size, size)], sem.at[t, p])
              for p in range(parts) for t, (src, dst) in enumerate(((a, a_out), (b, b_out), (c, c_out)))]
    for copy in copies:
        copy.start()
    for copy in copies:
        copy.wait()


def solution(mesh):
    n = mesh.shape['sp']
    row_spec = P('dp', 'sp', None)
    cache_spec = P('dp', 'sp', None, None)
    vec_spec = P(None)
    mat_spec = P(None, None)

    def local_layer(hidden, seq_lens, ln1_gain, ln1_bias, ln2_gain, ln2_bias, w_qkv, b_qkv, w_out, b_out, w_up, b_up, w_down, b_down):
        n_prompts, tok, d_model = hidden.shape
        hd = b_qkv.shape[2]
        d_ff = w_up.shape[1]
        seq = tok * n
        n_rows = n_prompts * tok
        n_chunks = n_prompts // PC
        rows = PC * tok
        fb = min(FB, d_ff // n_chunks)
        n_far = n // 2 - 3
        bf, f32 = jnp.bfloat16, jnp.float32
        row = lambda v: v.reshape(1, d_model)
        tabs = jnp.asarray(rotary_tables(seq, hd))
        cache = jax.ShapeDtypeStruct((n_prompts, 1, seq, hd), bf)
        like_out = jax.ShapeDtypeStruct((n_prompts, tok, d_model), bf)
        dma = pltpu.SemaphoreType.DMA
        q, k, v, out, _ = pl.pallas_call(
            functools.partial(layer_kernel, n),
            name='layer',
            out_shape=(cache, pltpu.VMEM(cache.shape, bf), pltpu.VMEM(cache.shape, bf), pltpu.VMEM(like_out.shape, bf),
                       jax.ShapeDtypeStruct((2, n_rows, d_model), bf)),
            in_specs=[SM, ANY, VM, VM, VM, VM, ANY, VM, ANY, ANY, VM, ANY, VM, ANY, VM],
            out_specs=(ANY, VM, VM, VM, ANY),
            scratch_shapes=[
                pltpu.VMEM((n_rows, d_model), bf),
                pltpu.VMEM((2, n_rows, d_model), bf),
                pltpu.VMEM((n_prompts, tok, d_model), bf),
                pltpu.VMEM((n_rows, d_model), f32),
                pltpu.VMEM((W_SLOTS, d_model, 3 * hd), bf),
                pltpu.VMEM((2, d_model, fb), bf),
                pltpu.VMEM((2, fb, d_model), bf),
                pltpu.VMEM((2, 2 * n_far + 6, 3, PC, tok, hd), bf),
                pltpu.VMEM((PC, seq - 2 * HOME * tok, hd), bf),
                pltpu.VMEM((2, PC, seq - 2 * HOME * tok, hd), bf),
                pltpu.VMEM((n, n_prompts, tok, hd), bf),
                pltpu.VMEM((2, rows, d_model), bf),
                pltpu.VMEM((2, 2, PC, tok, hd), bf), pltpu.VMEM((2, 4, PC, tok, hd), bf), pltpu.VMEM((2, 4, PC, tok, hd), bf),
                pltpu.VMEM((2, n // 2, PC, tok, hd), bf),
                pltpu.VMEM((5, 3, tok, hd), f32),
                dma((n_chunks,)), dma((W_SLOTS,)), dma((2,)), dma((2,)), dma((2, n_chunks)), dma((2, n_chunks)),
                dma((2, 2)), dma((2, 2)), dma((3, n_chunks)), dma(()), dma((2,)), dma((n_chunks,)), dma((2, d_model // fb)),
                dma((2, n_chunks)), dma((2, n_chunks)), dma((2,)), dma((2,)), dma((5,)),
            ],
            compiler_params=pltpu.CompilerParams(collective_id=0, has_side_effects=True, vmem_limit_bytes=VMEM_LIMIT),
            cost_estimate=pl.CostEstimate(flops=2 * n_rows * d_model * (4 * d_model + 2 * d_ff), bytes_accessed=200_000_000, transcendentals=0),
        )(seq_lens, hidden, row(ln1_gain), row(ln1_bias), row(ln2_gain), row(ln2_bias), w_qkv, jnp.transpose(b_qkv, (1, 0, 2)), tabs,
          w_up, b_up.reshape(d_ff // fb, 1, fb), w_down, row(b_down), w_out, row(b_out))
        parts = 4
        return pl.pallas_call(
            hand_on_kernel,
            name='hand_on',
            out_shape=(like_out, cache, cache),
            in_specs=[VM] * 3,
            out_specs=(ANY,) * 3,
            scratch_shapes=[dma((3, parts))],
            compiler_params=pltpu.CompilerParams(vmem_limit_bytes=1 << 20),
        )(*(pltpu.with_memory_space_constraint(t, pltpu.VMEM) for t in (out, k, v)))

    return jax.shard_map(local_layer, mesh=mesh,
                         in_specs=(row_spec, P('dp'), vec_spec, vec_spec, vec_spec, vec_spec, mat_spec, P(None, None, None), mat_spec, vec_spec, mat_spec, vec_spec, mat_spec, vec_spec),
                         out_specs=(row_spec, cache_spec, cache_spec), check_vma=False)
```
